512 devices in a mesh: blk: 32 (over x, y, z_hi), rel: 16 (over z_lo, core).
Axes of the slice: x: 4, y: 4, z: 16 (z_hi: 2, z_lo: 8; z = z_hi * 8 + z_lo), core: 2. Of those that a mesh axis runs over, the one named last changes fastest.
Arguments:
- features: bfloat16 [16384, 512], P(('blk', 'rel')), may hold values from -6 to 6
- adjacency: int32 [6, 512, 16, 1024], P(None, 'blk', 'rel'), may hold values from -2147483648 to 2147483646, as said below
- tile_mask: int32 [6, 128, 32, 16], P(None, 'blk', None, 'rel'), may hold values from 0 to 1
- bases: bfloat16 [512, 8, 512], P('rel'), may hold values from -0.25 to 0.25
- coefficients: float32 [6, 8], replicated, may hold values from -2 to 2
- self_weight: bfloat16 [512, 512], P('rel'), may hold values from -0.25 to 0.25
Outputs:
- updated: bfloat16 [16384, 512], P(('blk', 'rel'))
The draws below stay inside these ranges and needn't reach their ends.
Inputs may be any that keep to these rules, and one draw needn't show every extreme that they name: `adjacency`: each word holds 32 edge bits, bit t for destination node 32 * word index + t.
All inputs are finite; a program needn't handle non-finite values.
Results may differ from the reference program's by a relative error of at most 0.0058.
Values may be sent and summed in bfloat16 or wider, within the bound.
A program may use at most 64 MiB of HBM per device.

```python
import jax
import jax.numpy as jnp
from jax import lax

D = 512
RELS = 6
BASES = 8
NODE_DEV = 512
NODES = 16384
SUB = 32
N_BLK = 32
N_REL = 16


def draw_adjacency(key, part):
    shape = (RELS, NODES // 32, N_REL, N_BLK * SUB)
    first = jax.random.randint(jax.random.fold_in(key, 31), shape, -2147483648, 2147483647, dtype=jnp.int32)
    second = jax.random.randint(jax.random.fold_in(key, 37), shape, -2147483648, 2147483647, dtype=jnp.int32)
    third = jax.random.randint(jax.random.fold_in(key, 41), shape, -2147483648, 2147483647, dtype=jnp.int32)
    return jnp.bitwise_and(jnp.bitwise_and(first, second), third)


def draw_tile_mask(key, part):
    rate_key = jax.random.fold_in(key, 11)
    dense_key = jax.random.fold_in(key, 13)
    pick_key = jax.random.fold_in(key, 17)
    value_key = jax.random.fold_in(key, 23)
    sparse_rates = jax.random.randint(rate_key, (RELS, NODES // 128, 1, 1), 2, 26)
    dense_rates = jax.random.randint(dense_key, (RELS, NODES // 128, 1, 1), 30, 61)
    picked = jax.random.randint(pick_key, (RELS, NODES // 128, 1, 1), 0, 8) == 0
    rates = jnp.where(picked, dense_rates, sparse_rates)
    values = jax.random.randint(value_key, (RELS, NODES // 128, N_BLK, N_REL), 0, 100)
    return (values < rates).astype(jnp.int32)


def shard_levels(key, shape, pieces, low, high):
    def one(dim, parts):
        draws = jax.random.uniform(jax.random.fold_in(jax.random.fold_in(key, 6), dim), (parts,), jnp.float32, low / len(pieces), high / len(pieces))
        return jnp.repeat(jnp.exp(draws), shape[dim] // parts).reshape((-1,) + (1,) * (len(shape) - dim - 1))

    loudness = one(*pieces[0])
    for cut in pieces[1:]:
        loudness = loudness * one(*cut)
    return loudness


def normal_values(rng, dims, deviation, limit, cuts=(), kind=jnp.bfloat16):
    level = shard_levels(rng, dims, cuts, -0.22, 0.18) if cuts else 1.0
    result = jax.random.normal(rng, dims, jnp.float32) * deviation * level
    return jnp.minimum(jnp.maximum(result, -limit), limit).astype(kind)


def setup_inputs(seed: int = 0) -> dict:
    arg_keys = jax.random.split(jax.random.key(seed), 7)
    return {
        "features": normal_values(arg_keys[0], (NODES, D), 1.0, 6.0, ((0, 512),)),
        "adjacency": draw_adjacency(jax.random.fold_in(arg_keys[6], 71), 0),
        "tile_mask": draw_tile_mask(jax.random.fold_in(arg_keys[6], 71), 0),
        "bases": normal_values(arg_keys[3], (D, BASES, D), D ** -0.5, 0.25, ((0, 16),)),
        "coefficients": normal_values(arg_keys[4], (RELS, BASES), 0.35, 2.0, (), jnp.float32),
        "self_weight": normal_values(arg_keys[5], (D, D), D ** -0.5, 0.25, ((0, 16),)),
    }


def expand_edges(packed, tile_flags):
    shifts = jnp.arange(32, dtype=jnp.int32)
    edge_bits = jnp.bitwise_and(jnp.right_shift(packed[:, :, None, :], shifts[None, None, :, None]), 1)
    edge_bits = edge_bits.reshape(packed.shape[0], packed.shape[1] * 32, packed.shape[2])
    tile_rows = jnp.repeat(tile_flags, 128, axis=1)
    return edge_bits * tile_rows

def reference(features, adjacency, tile_mask, bases, coefficients, self_weight):
    relations = adjacency.shape[0]
    width = features.shape[1]
    rel_weight = jnp.einsum('rb,ibj->irj', coefficients.astype(jnp.float32), bases.astype(jnp.float32), precision=lax.Precision.HIGHEST).astype(jnp.bfloat16)
    projected = jnp.dot(features, rel_weight.reshape(width, relations * width), preferred_element_type=jnp.float32)
    projected = projected.astype(jnp.bfloat16).reshape(NODES, relations, width)
    reordered = adjacency.reshape(relations, NODES // 32, N_REL, N_BLK, SUB)
    reordered = jnp.transpose(reordered, (0, 1, 3, 2, 4))
    packed_all = reordered.reshape(relations, NODES // 32, N_BLK, NODE_DEV)
    flags_all = jnp.repeat(tile_mask, SUB, axis=3)

    def one_block(carry, block):
        running, degree = carry
        packed = lax.dynamic_index_in_dim(packed_all, block, 2, keepdims=False)
        flags = lax.dynamic_index_in_dim(flags_all, block, 2, keepdims=False)
        edges = expand_edges(packed, flags).astype(jnp.float32)
        values = lax.dynamic_slice_in_dim(projected, (block * NODE_DEV).astype(jnp.int32), NODE_DEV, 0).astype(jnp.float32)
        running = running + jnp.einsum('rns,srd->nd', edges, values)
        degree = degree + lax.optimization_barrier(jnp.sum(edges, axis=(0, 2)))
        return ((running, degree), None)
    start = (jnp.zeros((NODES, width), jnp.float32), jnp.zeros((NODES,), jnp.float32))
    (message, degree), _ = lax.scan(one_block, start, jnp.arange(N_BLK, dtype=jnp.int32))
    own = jnp.dot(features, self_weight, preferred_element_type=jnp.float32)
    return jax.nn.relu(own + message * lax.rsqrt(1.0 + degree)[:, None]).astype(jnp.bfloat16)
```

```python
import jax
import jax.numpy as jnp
from jax import lax
from jax.experimental import pallas as pl
from jax.experimental.pallas import tpu as pltpu
from jax.sharding import Mesh
from jax.sharding import PartitionSpec as P

AXES = ("x", "y", "h", "z", "p")
BLK = ("x", "y", "h")
REL = ("z", "p")
F32 = jnp.float32
BF16 = jnp.bfloat16
MESH = pl.DeviceIdType.MESH
SHIFTS = (1, -1, 2, -2, 3, -3, 4)


def kernel(feat_hbm, adj_hbm, mask_hbm, bases_hbm, coef, self_hbm, out_ref,
           feats, adj, mask, bases, own_self, weights, words, flags, edges, partial, counts,
           transit, deg_mine, deg_pair, deg_sum, deg_all, total, pair_out, pair_in, level_out, level_in,
           cross_out, cross_in, load_sem, send_sem, recv_sem):
    x, y, h, z, p = [lax.axis_index(a) for a in AXES]
    g = h * 8 + z
    row = 2 * z + p
    q = 1 - p

    def along_z(d):
        t = lax.rem(g + d + 16, 16)
        return (x, y, lax.div(t, 8), lax.rem(t, 8), p)

    def mate_first(m):
        return (lax.rem(x + m * q, 4), lax.rem(y + m * p, 4), h, z, p)

    def mate_second(m):
        return (lax.rem(x + m * p, 4), lax.rem(y + m * q, 4), h, z, p)

    sibling = (x, y, h, z, q)

    def slot(half, xx, yy):
        return feats.at[half, xx, lax.rem(yy, 2) * 2 + lax.div(yy, 2)]

    loads = []
    for i, (src, dst) in enumerate((
        (bases_hbm, bases), (feat_hbm, slot(h, x, y)), (self_hbm, own_self),
        (adj_hbm, adj), (mask_hbm, mask),
    )):
        copy = pltpu.make_async_copy(src, dst, load_sem.at[i])
        copy.start()
        loads.append(copy)

    barrier = pltpu.get_barrier_semaphore()
    greeted = [sibling]
    for m in (1, 2, 3):
        greeted += [mate_first(m), mate_second(m)]
    for d in (1, 2, 3, 4):
        greeted += [along_z(d), along_z(-d)]
    for device in greeted:
        pl.semaphore_signal(barrier, inc=1, device_id=device, device_id_type=MESH)

    started = []

    def send(src, dst, device):
        k = len(started)
        copy = pltpu.make_async_remote_copy(
            src_ref=src, dst_ref=dst, send_sem=send_sem.at[k], recv_sem=recv_sem.at[k],
            device_id=device, device_id_type=MESH)
        copy.start()
        started.append(copy)
        return copy

    lane = lax.broadcasted_iota(jnp.int32, (32, 256), 1)
    line = lax.broadcasted_iota(jnp.int32, (32, 256), 0)
    basis_of = lax.rem(lane, 8)
    own_row = lax.div(lane, 8) == line
    tops, mids, lows = [], [], []
    for r in range(6):
        values = jnp.zeros((32, 256), F32)
        for b in range(8):
            values = jnp.where(basis_of == b, coef[r, b], values)
        values = jnp.where(own_row, values, 0.0)
        top = values.astype(BF16)
        rest = values - top.astype(F32)
        mid = rest.astype(BF16)
        tops.append(top)
        mids.append(mid)
        lows.append((rest - mid.astype(F32)).astype(BF16))
    loads[0].wait()
    loads[2].wait()
    rows = bases[...]
    for r in range(6):
        made = (jnp.dot(lows[r], rows, preferred_element_type=F32)
                + jnp.dot(mids[r], rows, preferred_element_type=F32)
                + jnp.dot(tops[r], rows, preferred_element_type=F32)).astype(BF16)
        for s in range(4):
            weights[s, row, r] = made[:, 128 * s:128 * s + 128]
    for s in range(4):
        weights[s, row, 6] = own_self[:, 128 * s:128 * s + 128]

    loads[3].wait()
    loads[4].wait()
    flags[...] = jnp.zeros((128, 128), F32)
    for r in range(6):
        flags[4 * r:4 * r + 4, 0:32] = mask[r].astype(F32)
    pick = (lax.div(lax.broadcasted_iota(jnp.int32, (96, 128), 0), 4)
            == lax.broadcasted_iota(jnp.int32, (96, 128), 1)).astype(BF16)
    spread = (lax.div(lax.broadcasted_iota(jnp.int32, (128, 1024), 1), 32)
              == lax.broadcasted_iota(jnp.int32, (128, 1024), 0)).astype(BF16)
    per_word = jnp.dot(pick, flags[...].astype(BF16), preferred_element_type=F32).astype(BF16)
    keep = jnp.dot(per_word, spread, preferred_element_type=F32)
    odd = lax.rem(lax.div(lax.broadcasted_iota(jnp.int32, (16, 128), 1), 32), 2) == 1
    for r in range(6):
        for c in range(4):
            at = 256 * c
            first = jnp.where(keep[16 * r:16 * r + 16, at:at + 128] > 0.5, adj[r, :, 0, at:at + 128], 0)
            second = jnp.where(keep[16 * r:16 * r + 16, at + 128:at + 256] > 0.5, adj[r, :, 0, at + 128:at + 256], 0)
            words[0, r, :, 128 * c:128 * c + 128] = jnp.where(odd, pltpu.roll(second, 32, 1), first)
            words[1, r, :, 128 * c:128 * c + 128] = jnp.where(odd, second, pltpu.roll(first, 96, 1))
    counts[...] = jnp.zeros((512, 128), jnp.int32)
    loads[1].wait()

    pl.semaphore_wait(barrier, len(greeted))

    mine = slot(h, x, y)
    hop_a = send(mine.at[0:16], transit.at[0], along_z(4))
    hop_b = send(mine.at[16:32], transit.at[1], along_z(-4))
    own_first = [send(mine, mine, mate_first(m)) for m in (1, 2, 3)]
    quarter = x * q + y * p
    z_copies = []
    for d in SHIFTS:
        shift = d if d != 4 else 4 - 8 * p
        z_copies.append(send(weights.at[quarter, row], weights.at[quarter, row], along_z(shift)))
    pair_copies = [send(weights.at[s, row], weights.at[s, row], sibling) for s in range(4)]

    def expand(half):
        shifts = lax.broadcasted_iota(jnp.int32, (32, 512), 0)

        def one(r, carry):
            packed = words[half, r]
            for w in range(16):
                bits = jnp.bitwise_and(jnp.right_shift(jnp.broadcast_to(packed[w:w + 1, :], (32, 512)), shifts), 1)
                edges[half, r, 32 * w:32 * w + 32, :] = bits.astype(F32).astype(BF16)
                counts[32 * w:32 * w + 32, :] += (
                    (bits[:, 0:128] + bits[:, 128:256]) + (bits[:, 256:384] + bits[:, 384:512]))
            return carry

        lax.fori_loop(0, 6, one, 0)

    def second_turn(half, first):
        sent = []
        for m in (0, 1, 2, 3):
            if m:
                first[m - 1].wait_recv()
            part = slot(half, lax.rem(x - m * q + 4, 4), lax.rem(y - m * p + 4, 4))
            sent += [send(part, part, mate_second(k)) for k in (1, 2, 3)]
        return sent

    expand(h)
    own_second = second_turn(h, own_first)
    hop_a.wait_recv()
    behind = lax.div(lax.rem(g + 12, 16), 8)
    end_a = send(transit.at[0], slot(behind, x, y).at[0:16], along_z(4))
    hop_b.wait_recv()
    ahead = lax.div(lax.rem(g + 4, 16), 8)
    end_b = send(transit.at[1], slot(ahead, x, y).at[16:32], along_z(-4))

    xy_copies = []

    def forward_z(k):
        d = SHIFTS[k]
        z_copies[k].wait_recv()
        shift = d if d != 4 else 4 - 8 * p
        source = lax.rem(lax.rem(g - shift + 16, 16), 8) * 2 + p
        part = weights.at[quarter, source]
        xy_copies.append([(m, source, send(part, part, mate_first(m))) for m in (1, 2, 3)])
        pair_copies.append(send(part, part, sibling))

    def forward_xy(k):
        for m, source, copy in xy_copies[k]:
            copy.wait_recv()
            part = weights.at[lax.rem(quarter - m + 4, 4), source]
            pair_copies.append(send(part, part, sibling))

    other = 1 - h
    expand(other)
    forward_z(0)
    forward_z(1)

    ones = jnp.ones((8, 128), BF16)
    for c in range(4):
        deg_mine[c] = lax.dot_general(
            ones, counts[128 * c:128 * c + 128, :].astype(F32).astype(BF16), (((1,), (1,)), ((), ())),
            preferred_element_type=F32)
    deg_copy = send(deg_mine, deg_pair, sibling)

    for copy in own_second:
        copy.wait_recv()
    held = feats[h].reshape(512, 512)
    for r in range(6):
        partial[r] = jnp.dot(edges[h, r], held, preferred_element_type=F32)
    forward_z(2)
    forward_z(3)
    deg_copy.wait_recv()
    deg_sum[...] = deg_mine[...] + deg_pair[...]
    deg_copies = []
    for m in range(1, 8):
        zz = lax.rem(z + m, 8)
        deg_copies.append(send(deg_sum.at[lax.div(zz, 2)], deg_all.at[m], (x, y, h, zz, p)))
    deg_all[0] = deg_sum[lax.div(z, 2)]

    end_a.wait_recv()
    end_b.wait_recv()
    far = slot(other, x, y)
    far_first = [send(far, far, mate_first(m)) for m in (1, 2, 3)]
    forward_z(4)
    forward_z(5)
    far_second = second_turn(other, far_first)
    forward_z(6)
    for k in range(7):
        forward_xy(k)
    for copy in far_second:
        copy.wait_recv()
    for copy in pair_copies:
        copy.wait_recv()

    far_held = feats[other].reshape(512, 512)

    def weight(r):
        return jnp.concatenate([weights[s, :, r].reshape(512, 128) for s in range(4)], axis=1)

    side = lax.div(z, 4)
    place = lax.rem(z, 4)

    def group(turn, which):
        at = pl.ds(pl.multiple_of(which * 256, 256), 256)
        for r in range(6):
            a = (partial[r, at, :] + jnp.dot(edges[other, r, at, :], far_held, preferred_element_type=F32)).astype(BF16)
            term = jnp.dot(a, weight(r), preferred_element_type=F32).reshape(4, 2, 32, 512)
            if r == 0:
                total[turn] = term
            else:
                total[turn] += term
        pair_out[turn] = total[turn, :, q].astype(BF16)
        pair = send(pair_out.at[turn], pair_in.at[turn], sibling)
        return pair

    def level_sends(turn, pair):
        pair.wait_recv()
        total[turn, :, p] += pair_in[turn].astype(F32)
        level_out[turn] = total[turn, :, p].astype(BF16)
        sent = []
        for m in (1, 2, 3):
            i = lax.rem(place + m, 4)
            sent.append(send(level_out.at[turn, i], level_in.at[turn, m - 1], (x, y, h, side * 4 + i, p)))
        return sent

    def level_sum(turn, sent):
        for copy in sent:
            copy.wait_recv()
        value = total[turn, place, p]
        for m in range(3):
            value += level_in[turn, m].astype(F32)
        return value

    pair_far = group(0, 1 - side)
    level_far = level_sends(0, pair_far)
    pair_near = group(1, side)
    cross_out[...] = level_sum(0, level_far).astype(BF16)
    cross = send(cross_out, cross_in, (x, y, h, (1 - side) * 4 + place, p))
    level_near = level_sends(1, pair_near)

    own = jnp.dot(mine[...], weight(6), preferred_element_type=F32)
    for copy in deg_copies:
        copy.wait_recv()
    degrees = deg_all[0]
    for m in range(1, 8):
        degrees += deg_all[m]
    place_of = (lax.broadcasted_iota(jnp.int32, (32, 128), 1)
                == lax.rem(row, 4) * 32 + lax.broadcasted_iota(jnp.int32, (32, 128), 0))
    degree = jnp.sum(jnp.where(place_of, jnp.broadcast_to(degrees[0:1, :], (32, 128)), 0.0), axis=1, keepdims=True)
    scale = lax.rsqrt(1.0 + degree)
    message = level_sum(1, level_near)
    cross.wait_recv()
    message += cross_in[...].astype(F32)
    out_ref[...] = jnp.maximum(own + message * scale, 0.0).astype(BF16)
    for copy in started:
        copy.wait_send()


def shards(features, adjacency, tile_mask, bases, coefficients, self_weight):
    hbm = pl.BlockSpec(memory_space=pltpu.HBM)
    n = 160
    return pl.pallas_call(
        kernel,
        out_shape=jax.ShapeDtypeStruct((32, 512), BF16),
        in_specs=[hbm, hbm, hbm, hbm, pl.BlockSpec(memory_space=pltpu.SMEM), hbm],
        out_specs=pl.BlockSpec(memory_space=pltpu.VMEM),
        scratch_shapes=[
            pltpu.VMEM((2, 4, 4, 32, 512), BF16),
            pltpu.VMEM((6, 16, 1, 1024), jnp.int32),
            pltpu.VMEM((6, 4, 32), jnp.int32),
            pltpu.VMEM((256, 512), BF16),
            pltpu.VMEM((32, 512), BF16),
            pltpu.VMEM((4, 16, 7, 32, 128), BF16),
            pltpu.VMEM((2, 6, 16, 512), jnp.int32),
            pltpu.VMEM((128, 128), F32),
            pltpu.VMEM((2, 6, 512, 512), BF16),
            pltpu.VMEM((6, 512, 512), F32),
            pltpu.VMEM((512, 128), jnp.int32),
            pltpu.VMEM((2, 16, 512), BF16),
            pltpu.VMEM((4, 8, 128), F32),
            pltpu.VMEM((4, 8, 128), F32),
            pltpu.VMEM((4, 8, 128), F32),
            pltpu.VMEM((8, 8, 128), F32),
            pltpu.VMEM((2, 4, 2, 32, 512), F32),
            pltpu.VMEM((2, 4, 32, 512), BF16),
            pltpu.VMEM((2, 4, 32, 512), BF16),
            pltpu.VMEM((2, 4, 32, 512), BF16),
            pltpu.VMEM((2, 3, 32, 512), BF16),
            pltpu.VMEM((32, 512), BF16),
            pltpu.VMEM((32, 512), BF16),
            pltpu.SemaphoreType.DMA((5,)),
            pltpu.SemaphoreType.DMA((n,)),
            pltpu.SemaphoreType.DMA((n,)),
        ],
        compiler_params=pltpu.CompilerParams(
            collective_id=0, has_side_effects=True, vmem_limit_bytes=56 * 1024 * 1024),
    )(features, adjacency, tile_mask.reshape(6, 4, 32), bases.reshape(256, 512), coefficients, self_weight)


def solution(mesh):
    torus = Mesh(mesh.devices.reshape(4, 4, 2, 8, 2), AXES)
    placed = (
        P(AXES, None),
        P(None, BLK, REL, None),
        P(None, BLK, None, REL),
        P(REL, None, None),
        P(),
        P(REL, None),
    )
    return jax.shard_map(
        shards, mesh=torus, in_specs=placed, out_specs=P(AXES, None), check_vma=False
    )
```

```python
import jax
import jax.numpy as jnp
from jax import lax
from jax.experimental import pallas as pl
from jax.experimental.pallas import tpu as pltpu
from jax.sharding import Mesh
from jax.sharding import PartitionSpec as P

AXES = ("x", "y", "h", "z", "p")
BLK = ("x", "y", "h")
REL = ("z", "p")
F32 = jnp.float32
BF16 = jnp.bfloat16
MESH = pl.DeviceIdType.MESH
SHIFTS = (1, -1, 2, -2, 3, -3, 4)


def kernel(feat_hbm, adj_hbm, mask_hbm, bases_hbm, coef_hbm, self_hbm, out_ref,
           feats, adj, mask, bases, coef, own_self, weights, words, flags, edges, partial, counts, summed,
           transit, deg_mine, deg_pair, deg_sum, deg_all, total, pair_out, pair_in, level_out, level_in,
           cross_out, cross_in, load_sem, send_sem, recv_sem):
    x, y, h, z, p = [lax.axis_index(a) for a in AXES]
    g = h * 8 + z
    row = 2 * z + p
    q = 1 - p

    def along_z(d):
        t = lax.rem(g + d + 16, 16)
        return (x, y, lax.div(t, 8), lax.rem(t, 8), p)

    def mate_first(m):
        return (lax.rem(x + m * q, 4), lax.rem(y + m * p, 4), h, z, p)

    def mate_second(m):
        return (lax.rem(x + m * p, 4), lax.rem(y + m * q, 4), h, z, p)

    sibling = (x, y, h, z, q)

    def slot(half, xx, yy):
        return feats.at[half, xx, lax.rem(yy, 2) * 2 + lax.div(yy, 2)]

    barrier = pltpu.get_barrier_semaphore()
    greeted = [sibling]
    for d in (4, 3, 2, 1):
        greeted += [along_z(d), along_z(-d)]
    for m in (2, 1, 3):
        greeted += [mate_first(m), mate_second(m)]
    for device in greeted:
        pl.semaphore_signal(barrier, inc=1, device_id=device, device_id_type=MESH)
    mine = slot(h, x, y)
    loads = []
    for i, (src, dst) in enumerate((
        (feat_hbm, mine), (coef_hbm, coef), (bases_hbm, bases), (self_hbm, own_self),
        (mask_hbm, mask), (adj_hbm, adj),
    )):
        copy = pltpu.make_async_copy(src, dst, load_sem.at[i])
        copy.start()
        loads.append(copy)

    started = []

    def send(src, dst, device):
        k = len(started)
        copy = pltpu.make_async_remote_copy(
            src_ref=src, dst_ref=dst, send_sem=send_sem.at[k], recv_sem=recv_sem.at[k],
            device_id=device, device_id_type=MESH)
        copy.start()
        started.append(copy)
        return copy

    loads[0].wait()
    pl.semaphore_wait(barrier, len(greeted))
    hop_a = send(mine.at[0:16], transit.at[0], along_z(4))
    hop_b = send(mine.at[16:32], transit.at[1], along_z(-4))

    def first_turn(part):
        first = [send(part, part, mate_first(m)) for m in (2, 1, 3)]
        return first, [send(part, part, mate_second(m)) for m in (2, 1, 3)]

    def second_turn(half, first):
        sent = []
        for m, copy in zip((1, 3, 2), first[1:] + first[:1]):
            copy.wait_recv()
            part = slot(half, lax.rem(x - m * q + 4, 4), lax.rem(y - m * p + 4, 4))
            sent += [send(part, part, mate_second(k)) for k in (2, 1, 3)]
        return sent

    own_first, own_second = first_turn(mine)
    lane = lax.broadcasted_iota(jnp.int32, (32, 256), 1)
    loads[1].wait()
    line = lax.broadcasted_iota(jnp.int32, (32, 256), 0)
    basis_of = lax.rem(lane, 8)
    own_row = lax.div(lane, 8) == line
    tops, mids, lows = [], [], []
    for r in range(6):
        values = jnp.zeros((32, 256), F32)
        for b in range(8):
            values = jnp.where(basis_of == b, coef[r, b], values)
        values = jnp.where(own_row, values, 0.0)
        top = values.astype(BF16)
        rest = values - top.astype(F32)
        mid = rest.astype(BF16)
        tops.append(top)
        mids.append(mid)
        lows.append((rest - mid.astype(F32)).astype(BF16))
    loads[2].wait()
    loads[3].wait()
    rows = bases[...]
    for r in range(6):
        made = (jnp.dot(lows[r], rows, preferred_element_type=F32)
                + jnp.dot(mids[r], rows, preferred_element_type=F32)
                + jnp.dot(tops[r], rows, preferred_element_type=F32)).astype(BF16)
        for s in range(4):
            weights[s, row, r] = made[:, 128 * s:128 * s + 128]
    for s in range(4):
        weights[s, row, 6] = own_self[:, 128 * s:128 * s + 128]

    quarter = x * q + y * p
    z_copies = {}

    def send_z(d):
        shift = d if d != 4 else 4 - 8 * p
        z_copies[d] = send(weights.at[quarter, row], weights.at[quarter, row], along_z(shift))

    for d in (1, -1, 2, -2):
        send_z(d)
    pair_copies = [send(weights.at[s, row], weights.at[s, row], sibling) for s in range(4)]

    loads[4].wait()
    loads[5].wait()
    flags[...] = jnp.zeros((128, 128), F32)
    for r in range(6):
        flags[4 * r:4 * r + 4, 0:32] = mask[r].astype(F32)
    pick = (lax.div(lax.broadcasted_iota(jnp.int32, (96, 128), 0), 4)
            == lax.broadcasted_iota(jnp.int32, (96, 128), 1)).astype(BF16)
    spread = (lax.div(lax.broadcasted_iota(jnp.int32, (128, 1024), 1), 32)
              == lax.broadcasted_iota(jnp.int32, (128, 1024), 0)).astype(BF16)
    per_word = jnp.dot(pick, flags[...].astype(BF16), preferred_element_type=F32).astype(BF16)
    keep = jnp.dot(per_word, spread, preferred_element_type=F32)
    odd = lax.rem(lax.div(lax.broadcasted_iota(jnp.int32, (16, 128), 1), 32), 2) == 1
    for r in range(6):
        for c in range(4):
            at = 256 * c
            first = jnp.where(keep[16 * r:16 * r + 16, at:at + 128] > 0.5, adj[r, :, 0, at:at + 128], 0)
            second = jnp.where(keep[16 * r:16 * r + 16, at + 128:at + 256] > 0.5, adj[r, :, 0, at + 128:at + 256], 0)
            words[0, r, :, 128 * c:128 * c + 128] = jnp.where(odd, pltpu.roll(second, 32, 1), first)
            words[1, r, :, 128 * c:128 * c + 128] = jnp.where(odd, second, pltpu.roll(first, 96, 1))
    counts[...] = jnp.zeros((512, 128), jnp.int32)

    def expand(half):
        shifts = lax.broadcasted_iota(jnp.int32, (32, 512), 0)

        def one(r, carry):
            packed = words[half, r]
            for w in range(16):
                bits = jnp.bitwise_and(jnp.right_shift(jnp.broadcast_to(packed[w:w + 1, :], (32, 512)), shifts), 1)
                edges[half, r, 32 * w:32 * w + 32, :] = bits.astype(F32).astype(BF16)
                counts[32 * w:32 * w + 32, :] += (
                    (bits[:, 0:128] + bits[:, 128:256]) + (bits[:, 256:384] + bits[:, 384:512]))
            return carry

        lax.fori_loop(0, 6, one, 0)

    expand(h)
    hop_a.wait_recv()
    behind = lax.div(lax.rem(g + 12, 16), 8)
    end_a = send(transit.at[0], slot(behind, x, y).at[0:16], along_z(4))
    hop_b.wait_recv()
    ahead = lax.div(lax.rem(g + 4, 16), 8)
    end_b = send(transit.at[1], slot(ahead, x, y).at[16:32], along_z(-4))
    for d in (3, -3, 4):
        send_z(d)
    own_second += second_turn(h, own_first)

    xy_copies = {}

    def forward_z(d):
        z_copies[d].wait_recv()
        shift = d if d != 4 else 4 - 8 * p
        source = lax.rem(lax.rem(g - shift + 16, 16), 8) * 2 + p
        part = weights.at[quarter, source]
        xy_copies[d] = [(m, source, send(part, part, mate_first(m))) for m in (2, 1, 3)]
        pair_copies.append(send(part, part, sibling))

    def forward_xy(d):
        for m, source, copy in xy_copies[d]:
            copy.wait_recv()
            part = weights.at[lax.rem(quarter - m + 4, 4), source]
            pair_copies.append(send(part, part, sibling))

    for d in (1, -1, 2, -2):
        forward_z(d)
    other = 1 - h
    expand(other)
    ones = jnp.ones((8, 128), BF16)
    for c in range(4):
        deg_mine[c] = lax.dot_general(
            ones, counts[128 * c:128 * c + 128, :].astype(F32).astype(BF16), (((1,), (1,)), ((), ())),
            preferred_element_type=F32)
    deg_copy = send(deg_mine, deg_pair, sibling)
    end_a.wait_recv()
    end_b.wait_recv()
    far_first, far_second = first_turn(slot(other, x, y))
    for copy in own_second:
        copy.wait_recv()
    held = feats[h].reshape(512, 512)
    for r in range(6):
        partial[r] = jnp.dot(edges[h, r], held, preferred_element_type=F32)
    for d in (3, -3, 4):
        forward_z(d)
    far_second += second_turn(other, far_first)
    deg_copy.wait_recv()
    deg_sum[...] = deg_mine[...] + deg_pair[...]
    deg_copies = []
    for m in range(1, 8):
        zz = lax.rem(z + m, 8)
        deg_copies.append(send(deg_sum.at[lax.div(zz, 2)], deg_all.at[m], (x, y, h, zz, p)))
    deg_all[0] = deg_sum[lax.div(z, 2)]
    for d in SHIFTS:
        forward_xy(d)
    for copy in far_second:
        copy.wait_recv()
    far_held = feats[other].reshape(512, 512)

    def weight(r):
        return jnp.concatenate([weights[s, :, r].reshape(512, 128) for s in range(4)], axis=1)

    side = lax.div(z, 4)
    place = lax.rem(z, 4)

    def aggregate(turn, which):
        at = pl.ds(pl.multiple_of(which * 256, 256), 256)
        for r in range(6):
            summed[turn, r] = (partial[r, at, :] + jnp.dot(
                edges[other, r, at, :], far_held, preferred_element_type=F32)).astype(BF16)

    def transform(turn):
        for r in range(6):
            term = jnp.dot(summed[turn, r], weight(r), preferred_element_type=F32).reshape(4, 2, 32, 512)
            if r == 0:
                total[turn] = term
            else:
                total[turn] += term
        pair_out[turn] = total[turn, :, q].astype(BF16)
        return send(pair_out.at[turn], pair_in.at[turn], sibling)

    def partner(m):
        if m == 3:
            return 3 - place
        return lax.rem(place + 2, 4) if m == 2 else place + 1 - 2 * lax.rem(place, 2)

    def level_sends(turn, pair):
        pair.wait_recv()
        total[turn, :, p] += pair_in[turn].astype(F32)
        level_out[turn] = total[turn, :, p].astype(BF16)
        sent = []
        for m in (3, 2, 1):
            i = partner(m)
            sent.append(send(level_out.at[turn, i], level_in.at[turn, m - 1], (x, y, h, side * 4 + i, p)))
        return sent

    def level_sum(turn, sent):
        for copy in sent:
            copy.wait_recv()
        value = total[turn, place, p]
        for m in range(3):
            value += level_in[turn, m].astype(F32)
        return value

    aggregate(0, 1 - side)
    for copy in pair_copies:
        copy.wait_recv()
    pair_far = transform(0)
    aggregate(1, side)
    level_far = level_sends(0, pair_far)
    pair_near = transform(1)
    level_near = level_sends(1, pair_near)
    cross_out[...] = level_sum(0, level_far).astype(BF16)
    cross = send(cross_out, cross_in, (x, y, h, (1 - side) * 4 + place, p))
    own = jnp.dot(mine[...], weight(6), preferred_element_type=F32)
    for copy in deg_copies:
        copy.wait_recv()
    degrees = deg_all[0]
    for m in range(1, 8):
        degrees += deg_all[m]
    place_of = (lax.broadcasted_iota(jnp.int32, (32, 128), 1)
                == lax.rem(row, 4) * 32 + lax.broadcasted_iota(jnp.int32, (32, 128), 0))
    degree = jnp.sum(jnp.where(place_of, jnp.broadcast_to(degrees[0:1, :], (32, 128)), 0.0), axis=1, keepdims=True)
    scale = lax.rsqrt(1.0 + degree)
    message = level_sum(1, level_near)
    cross.wait_recv()
    message += cross_in[...].astype(F32)
    out_ref[...] = jnp.maximum(own + message * scale, 0.0).astype(BF16)
    for copy in started:
        copy.wait_send()


def shards(features, adjacency, tile_mask, bases, coefficients, self_weight):
    hbm = pl.BlockSpec(memory_space=pltpu.HBM)
    n = 160
    return pl.pallas_call(
        kernel,
        out_shape=jax.ShapeDtypeStruct((32, 512), BF16),
        in_specs=[hbm] * 6,
        out_specs=pl.BlockSpec(memory_space=pltpu.VMEM),
        scratch_shapes=[
            pltpu.VMEM((2, 4, 4, 32, 512), BF16),
            pltpu.VMEM((6, 16, 1, 1024), jnp.int32),
            pltpu.VMEM((6, 4, 32), jnp.int32),
            pltpu.VMEM((256, 512), BF16),
            pltpu.SMEM((6, 8), F32),
            pltpu.VMEM((32, 512), BF16),
            pltpu.VMEM((4, 16, 7, 32, 128), BF16),
            pltpu.VMEM((2, 6, 16, 512), jnp.int32),
            pltpu.VMEM((128, 128), F32),
            pltpu.VMEM((2, 6, 512, 512), BF16),
            pltpu.VMEM((6, 512, 512), F32),
            pltpu.VMEM((512, 128), jnp.int32),
            pltpu.VMEM((2, 6, 256, 512), BF16),
            pltpu.VMEM((2, 16, 512), BF16),
            pltpu.VMEM((4, 8, 128), F32),
            pltpu.VMEM((4, 8, 128), F32),
            pltpu.VMEM((4, 8, 128), F32),
            pltpu.VMEM((8, 8, 128), F32),
            pltpu.VMEM((2, 4, 2, 32, 512), F32),
            pltpu.VMEM((2, 4, 32, 512), BF16),
            pltpu.VMEM((2, 4, 32, 512), BF16),
            pltpu.VMEM((2, 4, 32, 512), BF16),
            pltpu.VMEM((2, 3, 32, 512), BF16),
            pltpu.VMEM((32, 512), BF16),
            pltpu.VMEM((32, 512), BF16),
            pltpu.SemaphoreType.DMA((6,)),
            pltpu.SemaphoreType.DMA((n,)),
            pltpu.SemaphoreType.DMA((n,)),
        ],
        compiler_params=pltpu.CompilerParams(
            collective_id=0, has_side_effects=True, vmem_limit_bytes=56 * 1024 * 1024),
    )(features, adjacency, tile_mask.reshape(6, 4, 32), bases.reshape(256, 512), coefficients, self_weight)


def solution(mesh):
    torus = Mesh(mesh.devices.reshape(4, 4, 2, 8, 2), AXES)
    placed = (
        P(AXES, None),
        P(None, BLK, REL, None),
        P(None, BLK, None, REL),
        P(REL, None, None),
        P(),
        P(REL, None),
    )
    return jax.shard_map(
        shards, mesh=torus, in_specs=placed, out_specs=P(AXES, None), check_vma=False
    )
```
